32 devices in a mesh: seq: 4 (over y, core), blk: 8 (over z, x).
Axes of the slice: x: 2, y: 2, z: 4, core: 2. Of those that a mesh axis runs over, the one named last changes fastest.
Arguments:
- kv_cache: bfloat16 [4, 2, 16, 4096, 1024], P(None, None, None, ('seq', 'blk')), may hold values from -18 to 18, as said below
- queries: bfloat16 [4, 128, 1024], P(None, 'blk'), may hold values from -400 to 400
- fresh_key_value: bfloat16 [4, 2, 128, 128], P(None, None, 'blk'), may hold values from -70 to 70
- lengths: int32 [16], replicated, may hold values from 1 to 4096, 49152 in all
Outputs:
- quant_cache: bfloat16 [4, 2, 128, 4096, 128], P(None, None, 'blk', 'seq')
- block_scale: float32 [4, 2, 128, 32], P(None, None, 'blk', 'seq')
- attended: bfloat16 [4, 128, 1024], P(None, 'blk')
The draws below stay inside these ranges and needn't reach their ends.
Inputs may be any that keep to these rules, and one draw needn't show every extreme that they name: `kv_cache`: each entry is a random value times a factor drawn for its position and head. `lengths`: every sequence has at least one live position, and some sequence uses all 4096.
All inputs are finite; a program needn't handle non-finite values.
Results may differ from the reference program's by a relative error of at most 0.003.
The reference program's roundings to bfloat16 on the way count: a program that leaves them out, or rounds other values in their place, can miss the bound.
Values may be sent and summed in bfloat16 or wider, within the bound.
A program may use at most 192 MiB of HBM per device.

```python
import math
import jax
import jax.numpy as jnp
import numpy as np
from jax import lax

KEY_VALUE_HEADS = 8
HEAD_DIM = 128
QUERY_GROUP = 8
SEQUENCE_COUNT = 16
CACHE_LENGTH = 4096
LAYER_COUNT = 4
BLOCK = 128


def draw_kv_cache(key, part):
    first_part, second_part = jax.random.split(jax.random.fold_in(key, 11))
    array_shape = (LAYER_COUNT, 2, SEQUENCE_COUNT, CACHE_LENGTH, KEY_VALUE_HEADS, HEAD_DIM)
    base_offset = jax.random.truncated_normal(first_part, -4.0, 4.0, array_shape, jnp.float32)
    scale_factor = jnp.exp(jax.random.uniform(second_part, (LAYER_COUNT, 2, SEQUENCE_COUNT, CACHE_LENGTH, KEY_VALUE_HEADS, 1), jnp.float32, -1.5, 1.5))
    return (base_offset * scale_factor).reshape(LAYER_COUNT, 2, SEQUENCE_COUNT, CACHE_LENGTH, KEY_VALUE_HEADS * HEAD_DIM).astype(jnp.bfloat16)


def draw_queries(key, part):
    first_part, second_part = jax.random.split(jax.random.fold_in(key, 23))
    base_offset = jax.random.truncated_normal(first_part, -6.0, 6.0, (LAYER_COUNT, KEY_VALUE_HEADS * SEQUENCE_COUNT, QUERY_GROUP, HEAD_DIM), jnp.float32)
    return base_offset.reshape(LAYER_COUNT, KEY_VALUE_HEADS * SEQUENCE_COUNT, QUERY_GROUP * HEAD_DIM).astype(jnp.bfloat16)


def draw_fresh_key_value(key, part):
    noise_key, value_key = jax.random.split(jax.random.fold_in(key, 37))
    query_rows = draw_queries(key, part).astype(jnp.float32)
    query_rows = query_rows.reshape(LAYER_COUNT, KEY_VALUE_HEADS * SEQUENCE_COUNT, QUERY_GROUP, HEAD_DIM)
    summed = jnp.sum(query_rows, axis=2)
    length = jnp.sqrt(jnp.sum(summed * summed, axis=-1, keepdims=True) + 1.0)
    noise = 0.5 * jax.random.normal(noise_key, summed.shape, jnp.float32)
    fresh_key = jnp.clip(5.0 * jnp.sqrt(jnp.float32(HEAD_DIM)) * summed / length + noise, -70.0, 70.0)
    fresh_value = jax.random.truncated_normal(value_key, -6.0, 6.0, summed.shape, jnp.float32)
    return jnp.stack([fresh_key, fresh_value], axis=1).astype(jnp.bfloat16)


def length_profile(number_of, total, limit, skew):
    weights = [(1 << 20) // math.isqrt(rank ** skew) + 1 for rank in range(2, number_of + 1)]
    spare, counts = total - limit - (number_of - 1), [1] * (number_of - 1)
    while spare > 0:
        candidates = [i for i in range(number_of - 1) if counts[i] < limit]
        pool, left = sum([weights[i] for i in candidates]), spare
        for i in candidates:
            more = min(limit - counts[i], max(1, left * weights[i] // pool), spare)
            counts[i] = counts[i] + more
            spare = spare - more
    return np.array([limit] + counts)


def ragged(stream_key, amount, total, reach, slope):
    if amount == 2:
        one = jax.random.randint(stream_key, (), max(1, total - reach), min(reach, total - 1) + 1)
        return jnp.stack([one, total - one])
    tallies = jnp.asarray(length_profile(amount, total, reach, slope), jnp.int32)
    pairs = (amount - 1) // 2
    source_of, taker = tallies[1:1 + 2 * pairs:2], tallies[2:2 + 2 * pairs:2]
    margin = jnp.minimum(source_of - 1, reach - taker)
    moved = jax.random.randint(jax.random.fold_in(stream_key, 1), (pairs,), 0, 1 << 20) % (margin + 1)
    tallies = tallies.at[1:1 + 2 * pairs:2].set(source_of - moved).at[2:2 + 2 * pairs:2].set(taker + moved)
    return tallies[jax.random.permutation(jax.random.fold_in(stream_key, 2), amount)]


def setup_inputs(seed: int = 0) -> dict:
    key_list = jax.random.split(jax.random.key(seed), 5)
    return {
        "kv_cache": draw_kv_cache(jax.random.fold_in(key_list[4], 71), 0),
        "queries": draw_queries(jax.random.fold_in(key_list[4], 71), 0),
        "fresh_key_value": draw_fresh_key_value(jax.random.fold_in(key_list[4], 71), 0),
        "lengths": ragged(key_list[3], SEQUENCE_COUNT, 3 * SEQUENCE_COUNT * CACHE_LENGTH // 4, CACHE_LENGTH, 1).astype(jnp.int32),
    }


def one_layer(lengths, items):
    cache, query, fresh = items
    seq_len = cache.shape[2]
    batch = cache.shape[1]
    heads = cache.shape[3] // HEAD_DIM
    blocks = seq_len // BLOCK
    values = cache.astype(jnp.float32).reshape(2, batch, blocks, BLOCK, heads, HEAD_DIM)
    scale = jnp.maximum(lax.optimization_barrier(jnp.max(jnp.abs(values), axis=(3, 5))), 1.0) / 127.0
    quant = (values / scale[:, :, :, None, :, None]).astype(jnp.bfloat16)
    quant = quant.transpose(0, 4, 1, 2, 3, 5).reshape(2, heads * batch, seq_len, HEAD_DIM)
    scale = scale.transpose(0, 3, 1, 2).reshape(2, heads * batch, blocks)
    rows = heads * batch
    inverse = 1.0 / jnp.sqrt(jnp.float32(HEAD_DIM))
    grouped = query.reshape(rows, QUERY_GROUP, HEAD_DIM).astype(jnp.float32)
    raw = jnp.einsum('pgd,prd->pgr', grouped, quant[0].astype(jnp.float32), precision=lax.Precision.HIGHEST)
    scores = raw.reshape(rows, QUERY_GROUP, blocks, BLOCK) * scale[0][:, None, :, None] * inverse
    pair_len = jnp.tile(lengths, heads)
    positions = jnp.arange(seq_len, dtype=jnp.int32).reshape(blocks, BLOCK)
    valid = positions[None] < pair_len[:, None, None]
    masked = jnp.where(valid[:, None], scores, -1e+30)
    peak = lax.optimization_barrier(jnp.max(masked, axis=-1))
    weight = jnp.where(valid[:, None], jnp.exp(masked - peak[..., None]), 0.0)
    total = lax.optimization_barrier(jnp.sum(weight, axis=-1))
    rounded = (weight * scale[1][:, None, :, None]).astype(jnp.bfloat16)
    part = jnp.einsum('pgnt,pntd->pgnd', rounded.astype(jnp.float32), quant[1].reshape(rows, blocks, BLOCK, HEAD_DIM).astype(jnp.float32), precision=lax.Precision.HIGHEST)
    own = jnp.einsum('pgd,pd->pg', grouped, fresh[0].astype(jnp.float32), precision=lax.Precision.HIGHEST) * inverse
    top = jnp.maximum(lax.optimization_barrier(jnp.max(peak, axis=-1)), own)
    scale_factor = jnp.exp(peak - top[..., None])
    own_w = jnp.exp(own - top)
    numer = lax.optimization_barrier(jnp.sum(scale_factor[..., None] * part, axis=2)) + own_w[..., None] * fresh[1].astype(jnp.float32)[:, None, :]
    denom = lax.optimization_barrier(jnp.sum(scale_factor * total, axis=-1)) + own_w
    attended = (numer / denom[..., None]).reshape(rows, QUERY_GROUP * HEAD_DIM).astype(jnp.bfloat16)
    return (quant, scale, attended)

def reference(kv_cache, queries, fresh_key_value, lengths):
    quant, scale, attended = lax.map(lambda items: one_layer(lengths, items), (kv_cache, queries, fresh_key_value))
    return (quant, scale, attended)
```

```python
import functools

import jax
import jax.numpy as jnp
from jax import lax
from jax.experimental import pallas as pl
from jax.experimental.pallas import tpu as pltpu
from jax.sharding import PartitionSpec as P

HEAD_DIM = 128
QUERY_GROUP = 8
BLOCK = 128
MESH = pl.DeviceIdType.MESH


def gather_kernel(x_ref, o_ref):
    o_ref[0] = x_ref[0]


def gather_parts(kv_cache, layer, s0, ns, owners):
    layers, _, batch, rows, width = kv_cache.shape
    pairs = (width // HEAD_DIM) * batch // owners

    def in_map(j):
        first = j * pairs + s0
        return (layer, 0, (first % batch) // ns, 0, first // batch)

    shape = (owners, 2, ns, rows, HEAD_DIM)
    size = owners * 2 * ns * rows * HEAD_DIM * 2
    return pl.pallas_call(
        gather_kernel,
        grid=(owners,),
        in_specs=[pl.BlockSpec((1, 2, ns, rows, HEAD_DIM), in_map)],
        out_specs=pl.BlockSpec((1, 2, ns, rows, HEAD_DIM), lambda j: (j, 0, 0, 0, 0)),
        out_shape=jax.ShapeDtypeStruct(shape, kv_cache.dtype),
        cost_estimate=pl.CostEstimate(flops=0, bytes_accessed=2 * size, transcendentals=0),
        compiler_params=pltpu.CompilerParams(vmem_limit_bytes=16 << 20),
    )(kv_cache)


def attend_kernel(s0, step_pairs, left_ref, x_ref, q_ref, *rest):
    quant_ref, scale_ref, stat_ref = rest[-3:]
    parts, _, _, rows, _ = x_ref.shape
    blocks = parts * rows // BLOCK
    inverse = 1.0 / (float(HEAD_DIM) ** 0.5)
    per_block = max(1, BLOCK // rows)
    lane = lax.broadcasted_iota(jnp.int32, (QUERY_GROUP, BLOCK), 1)
    lane_row = lax.broadcasted_iota(jnp.int32, (1, blocks), 1)

    def take(c, s, n):
        if rows >= BLOCK:
            inside = rows // BLOCK
            lo = (n % inside) * BLOCK
            return x_ref[n // inside, c, s, lo : lo + BLOCK, :]
        piece = x_ref[n * per_block : (n + 1) * per_block, c, s, :, :]
        return piece.reshape(BLOCK, HEAD_DIM)

    for s in range(step_pairs):
        live = left_ref[s0 + pl.program_id(0) * step_pairs + s]
        scales = [[], []]
        for c in range(2):
            row = jnp.zeros((1, blocks), jnp.float32)
            for n in range(blocks):
                piece = take(c, s, n)
                top = jnp.max(jnp.abs(piece), axis=0, keepdims=True)
                top = jnp.max(top.astype(jnp.float32), axis=1, keepdims=True)
                scale = jnp.maximum(top, 1.0) / 127.0
                quant = piece.astype(jnp.float32) * (1.0 / scale)
                quant_ref[0, c, s, n * BLOCK : (n + 1) * BLOCK, :] = quant.astype(jnp.bfloat16)
                scales[c].append(scale)
                row = jnp.where(lane_row == n, scale, row)
            scale_ref[s, c : c + 1, :] = row
        raw = lax.dot_general(
            q_ref[0, s],
            quant_ref[0, 0, s],
            (((1,), (1,)), ((), ())),
            preferred_element_type=jnp.float32,
        )
        peaks, totals, sums = [], [], []
        for n in range(blocks):
            score = raw[:, n * BLOCK : (n + 1) * BLOCK] * (scales[0][n] * inverse)
            valid = lane + n * BLOCK < live
            score = jnp.where(valid, score, -1e30)
            peak = jnp.max(score, axis=1, keepdims=True)
            weight = jnp.where(valid, jnp.exp(score - peak), 0.0)
            peaks.append(peak)
            totals.append(jnp.sum(weight, axis=1, keepdims=True))
            rounded = (weight * scales[1][n]).astype(jnp.bfloat16)
            sums.append(
                jnp.dot(
                    rounded,
                    quant_ref[0, 1, s, n * BLOCK : (n + 1) * BLOCK, :],
                    preferred_element_type=jnp.float32,
                )
            )
        top = functools.reduce(jnp.maximum, peaks)
        total = jnp.zeros_like(top)
        numer = jnp.zeros((QUERY_GROUP, HEAD_DIM), jnp.float32)
        for n in range(blocks):
            factor = jnp.exp(peaks[n] - top)
            total = total + factor * totals[n]
            numer = numer + factor * sums[n]
        stat_ref[s, 0] = numer
        stat_ref[s, 1] = jnp.where(lane < BLOCK // 2, top, total)


def attend(left, moved, queries, quant, out_shape, layer, s0):
    owners, _, ns, rows, _ = moved.shape
    seq_rows = owners * rows
    blocks = seq_rows // BLOCK
    step_pairs = 2 if ns % 2 == 0 else 1
    size = 2 * ns * seq_rows * HEAD_DIM * 2
    first = s0 // step_pairs
    in_specs = [
        pl.BlockSpec((owners, 2, step_pairs, rows, HEAD_DIM), lambda i, left: (0, 0, i, 0, 0)),
        pl.BlockSpec(
            (1, step_pairs, QUERY_GROUP, HEAD_DIM), lambda i, left: (layer, first + i, 0, 0)
        ),
    ]
    operands = [left, moved, queries]
    aliases = {}
    if quant is not None:
        in_specs.append(pl.BlockSpec(memory_space=pl.ANY))
        operands.append(quant)
        aliases = {3: 0}
    return pl.pallas_call(
        functools.partial(attend_kernel, s0, step_pairs),
        grid_spec=pltpu.PrefetchScalarGridSpec(
            num_scalar_prefetch=1,
            grid=(ns // step_pairs,),
            in_specs=in_specs,
            out_specs=[
                pl.BlockSpec(
                    (1, 2, step_pairs, seq_rows, HEAD_DIM),
                    lambda i, left: (layer, 0, first + i, 0, 0),
                ),
                pl.BlockSpec((step_pairs, 2, blocks), lambda i, left: (i, 0, 0)),
                pl.BlockSpec(
                    (step_pairs, 2, QUERY_GROUP, HEAD_DIM), lambda i, left: (i, 0, 0, 0)
                ),
            ],
        ),
        out_shape=[
            jax.ShapeDtypeStruct(out_shape, jnp.bfloat16),
            jax.ShapeDtypeStruct((ns, 2, blocks), jnp.float32),
            jax.ShapeDtypeStruct((ns, 2, QUERY_GROUP, HEAD_DIM), jnp.float32),
        ],
        input_output_aliases=aliases,
        cost_estimate=pl.CostEstimate(
            flops=4 * size * QUERY_GROUP, bytes_accessed=2 * size, transcendentals=0
        ),
        compiler_params=pltpu.CompilerParams(vmem_limit_bytes=24 << 20),
    )(*operands)


def combine_kernel(stat_ref, q_ref, fresh_ref, o_ref, held, send_sem, recv_sem):
    ranges = lax.axis_size("seq")
    me = lax.axis_index("seq")
    amount = stat_ref.shape[0]
    inverse = 1.0 / (float(HEAD_DIM) ** 0.5)
    barrier = pltpu.get_barrier_semaphore()
    for k in range(1, ranges):
        pl.semaphore_signal(
            barrier, inc=1, device_id={"seq": (me + k) % ranges}, device_id_type=MESH
        )
    pl.semaphore_wait(barrier, ranges - 1)
    copies = []
    for k in range(1, ranges):
        copy = pltpu.make_async_remote_copy(
            src_ref=stat_ref,
            dst_ref=held.at[me],
            send_sem=send_sem.at[k - 1],
            recv_sem=recv_sem.at[k - 1],
            device_id={"seq": (me + k) % ranges},
            device_id_type=MESH,
        )
        copy.start()
        copies.append(copy)
    held[me] = stat_ref[...]
    for copy in copies:
        copy.wait()

    def one(i, carry):
        query = q_ref[i].astype(jnp.float32)
        fresh_key = fresh_ref[i, 0:1, :]
        fresh_value = fresh_ref[i, 1:2, :]
        own = jnp.sum(query * fresh_key, axis=1, keepdims=True) * inverse
        tails = [held[r, i, 1] for r in range(ranges)]
        tops = [tail[:, 0:1] for tail in tails]
        top = functools.reduce(jnp.maximum, tops, own)
        own_weight = jnp.exp(own - top)
        numer = own_weight * fresh_value
        denom = own_weight
        for r in range(ranges):
            factor = jnp.exp(tops[r] - top)
            numer = numer + factor * held[r, i, 0]
            denom = denom + factor * tails[r][:, BLOCK // 2 : BLOCK // 2 + 1]
        o_ref[i] = (numer / denom).astype(jnp.bfloat16)
        return carry

    lax.fori_loop(0, amount, one, 0)


def combine(stat, queries, fresh, ident):
    amount = stat.shape[0]
    ranges = lax.axis_size("seq")
    return pl.pallas_call(
        combine_kernel,
        in_specs=[pl.BlockSpec(memory_space=pltpu.VMEM)] * 3,
        out_specs=pl.BlockSpec(memory_space=pltpu.VMEM),
        out_shape=jax.ShapeDtypeStruct((amount, QUERY_GROUP, HEAD_DIM), jnp.bfloat16),
        scratch_shapes=[
            pltpu.VMEM((ranges, *stat.shape), jnp.float32),
            pltpu.SemaphoreType.DMA((ranges - 1,)),
            pltpu.SemaphoreType.DMA((ranges - 1,)),
        ],
        cost_estimate=pl.CostEstimate(
            flops=0, bytes_accessed=stat.size * 4 * ranges, transcendentals=0
        ),
        compiler_params=pltpu.CompilerParams(
            collective_id=ident, has_side_effects=True, vmem_limit_bytes=16 << 20
        ),
    )(stat, queries, fresh)


def on_device(kv_cache, queries, fresh_key_value, lengths):
    layers, _, batch, rows, width = kv_cache.shape
    heads = width // HEAD_DIM
    owners = lax.axis_size("blk")
    pairs = heads * batch // owners
    seq_rows = rows * owners
    blocks = seq_rows // BLOCK
    first_pair = lax.axis_index("blk") * pairs
    left = lengths[(first_pair + jnp.arange(pairs, dtype=jnp.int32)) % batch]
    left = left - lax.axis_index("seq") * seq_rows
    grouped = queries.reshape(layers, pairs, QUERY_GROUP, HEAD_DIM)
    chunks = [(layer, 0, pairs) for layer in range(layers)]
    out_shape = (layers, 2, pairs, seq_rows, HEAD_DIM)

    quant = None
    scales, stats = [], []
    for layer, s0, ns in chunks:
        sent = gather_parts(kv_cache, layer, s0, ns, owners)
        moved = lax.all_to_all(sent, "blk", split_axis=0, concat_axis=0, tiled=True)
        quant, scale, stat = attend(left, moved, grouped, quant, out_shape, layer, s0)
        scales.append(scale)
        stats.append(stat)
    fresh = fresh_key_value.transpose(0, 2, 1, 3).astype(jnp.float32)
    early = layers - 1
    outs = []
    for ident, (lo, hi) in enumerate([(0, early), (early, layers)]):
        amount = (hi - lo) * pairs
        outs.append(
            combine(
                jnp.concatenate(stats[lo:hi], axis=0),
                grouped[lo:hi].reshape(amount, QUERY_GROUP, HEAD_DIM),
                fresh[lo:hi].reshape(amount, 2, HEAD_DIM),
                ident,
            ).reshape(hi - lo, pairs, QUERY_GROUP * HEAD_DIM)
        )
    attended = jnp.concatenate(outs, axis=0)
    block_scale = jnp.stack(scales).transpose(0, 2, 1, 3)
    return quant, block_scale, attended


def solution(mesh):
    in_specs = (
        P(None, None, None, ("seq", "blk"), None),
        P(None, "blk", None),
        P(None, None, "blk", None),
        P(),
    )
    out_specs = (
        P(None, None, "blk", "seq", None),
        P(None, None, "blk", "seq"),
        P(None, "blk", None),
    )
    return jax.shard_map(
        on_device, mesh=mesh, in_specs=in_specs, out_specs=out_specs, check_vma=False
    )
```

```python
import functools

import jax
import jax.numpy as jnp
from jax import lax
from jax.experimental import pallas as pl
from jax.experimental.pallas import tpu as pltpu
from jax.sharding import PartitionSpec as P

HEAD_DIM = 128
QUERY_GROUP = 8
BLOCK = 128
MESH = pl.DeviceIdType.MESH


def hand_over_kernel(
    kv_ref, moved_ref, tail_ref, own, held, send_sem, recv_sem, own_in, own_out, tail_in, tail_out
):
    owners = lax.axis_size("blk")
    me = lax.axis_index("blk")
    _, units, _, ns, _, _ = moved_ref.shape
    layers, _, batch, _, width = kv_ref.shape
    halves = (units + 1) // layers
    pairs = halves * ns

    def part(owner, unit):
        first = owner * pairs + (unit % halves) * ns
        head = pl.multiple_of((first // batch) * HEAD_DIM, HEAD_DIM)
        return kv_ref.at[
            unit // halves, :, pl.ds(first % batch, ns), :, pl.ds(head, HEAD_DIM)
        ]

    bits = owners.bit_length() - 1

    def partner(k):
        if owners != 1 << bits:
            return (me + k) % owners
        peer = me + k
        for b in range(bits):
            peer = peer - 2 * (1 << b) * ((me // (1 << b)) % 2) * ((k // (1 << b)) % 2)
        return peer

    def send(unit, k):
        peer = partner(k)
        return pltpu.make_async_remote_copy(
            src_ref=part(peer, unit),
            dst_ref=moved_ref.at[me, unit],
            send_sem=send_sem.at[unit, k - 1],
            recv_sem=recv_sem.at[unit, k - 1],
            device_id={"blk": peer},
            device_id_type=MESH,
        )

    def loop(lo, hi, act):
        def step(i, carry):
            act(i)
            return carry

        lax.fori_loop(lo, hi, step, 0)

    barrier = pltpu.get_barrier_semaphore()
    loop(
        1,
        owners,
        lambda k: pl.semaphore_signal(
            barrier, inc=1, device_id={"blk": (me + k) % owners}, device_id_type=MESH
        ),
    )
    pl.semaphore_wait(barrier, owners - 1)
    loop(0, units, lambda u: loop(1, owners, lambda k: send(u, k).start()))

    take_own = lambda u: pltpu.make_async_copy(part(me, u), own.at[u], own_in.at[u])
    give_own = lambda u: pltpu.make_async_copy(own.at[u], moved_ref.at[me, u], own_out.at[u])
    take_tail = lambda j: pltpu.make_async_copy(part(j, units), held.at[j], tail_in.at[j])
    give_tail = lambda j: pltpu.make_async_copy(held.at[j], tail_ref.at[j], tail_out.at[j])
    loop(0, owners, lambda j: take_tail(j).start())
    loop(0, units, lambda u: take_own(u).start())
    loop(0, owners, lambda j: take_tail(j).wait())
    loop(0, owners, lambda j: give_tail(j).start())
    loop(0, units, lambda u: take_own(u).wait())
    loop(0, units, lambda u: give_own(u).start())
    loop(0, owners, lambda j: give_tail(j).wait())
    loop(0, units, lambda u: give_own(u).wait())
    loop(0, units, lambda u: loop(1, owners, lambda k: send(u, k).wait()))


def hand_over(kv_cache, units, ns):
    rows = kv_cache.shape[3]
    owners = lax.axis_size("blk")
    piece = (2, ns, rows, HEAD_DIM)
    dtype = kv_cache.dtype
    dma = pltpu.SemaphoreType.DMA
    return pl.pallas_call(
        hand_over_kernel,
        in_specs=[pl.BlockSpec(memory_space=pl.ANY)],
        out_specs=[pl.BlockSpec(memory_space=pl.ANY)] * 2,
        out_shape=[
            jax.ShapeDtypeStruct((owners, units, *piece), dtype),
            jax.ShapeDtypeStruct((owners, *piece), dtype),
        ],
        scratch_shapes=[
            pltpu.VMEM((units, *piece), dtype),
            pltpu.VMEM((owners, *piece), dtype),
            dma((units, owners - 1)),
            dma((units, owners - 1)),
            dma((units,)),
            dma((units,)),
            dma((owners,)),
            dma((owners,)),
        ],
        cost_estimate=pl.CostEstimate(
            flops=0, bytes_accessed=4 * kv_cache.size, transcendentals=0
        ),
        compiler_params=pltpu.CompilerParams(
            collective_id=2, has_side_effects=True, vmem_limit_bytes=60 << 20
        ),
    )(kv_cache)


def attend_kernel(unit0, halves, ns, step_pairs, left_ref, x_ref, q_ref, *rest):
    quant_ref, scale_ref, stat_ref = rest[-3:]
    parts, _, _, _, rows, _ = x_ref.shape
    blocks = parts * rows // BLOCK
    inverse = 1.0 / (float(HEAD_DIM) ** 0.5)
    per_block = max(1, BLOCK // rows)
    lane = lax.broadcasted_iota(jnp.int32, (QUERY_GROUP, BLOCK), 1)
    lane_row = lax.broadcasted_iota(jnp.int32, (1, blocks), 1)

    def take(c, s, n):
        if rows >= BLOCK:
            inside = rows // BLOCK
            lo = (n % inside) * BLOCK
            return x_ref[n // inside, 0, c, s, lo : lo + BLOCK, :]
        piece = x_ref[n * per_block : (n + 1) * per_block, 0, c, s, :, :]
        return piece.reshape(BLOCK, HEAD_DIM)

    start = ((unit0 + pl.program_id(0)) % halves) * ns + pl.program_id(1) * step_pairs
    for s in range(step_pairs):
        live = left_ref[start + s]
        scales = [[], []]
        for c in range(2):
            row = jnp.zeros((1, blocks), jnp.float32)
            for n in range(blocks):
                piece = take(c, s, n)
                top = jnp.max(jnp.abs(piece), axis=0, keepdims=True)
                top = jnp.max(top.astype(jnp.float32), axis=1, keepdims=True)
                scale = jnp.maximum(top, 1.0) / 127.0
                quant = piece.astype(jnp.float32) * (1.0 / scale)
                quant_ref[0, c, s, n * BLOCK : (n + 1) * BLOCK, :] = quant.astype(jnp.bfloat16)
                scales[c].append(scale)
                row = jnp.where(lane_row == n, scale, row)
            scale_ref[s, c : c + 1, :] = row
        raw = lax.dot_general(
            q_ref[0, s],
            quant_ref[0, 0, s],
            (((1,), (1,)), ((), ())),
            preferred_element_type=jnp.float32,
        )
        peaks, totals, sums = [], [], []
        for n in range(blocks):
            score = raw[:, n * BLOCK : (n + 1) * BLOCK] * (scales[0][n] * inverse)
            valid = lane + n * BLOCK < live
            score = jnp.where(valid, score, -1e30)
            peak = jnp.max(score, axis=1, keepdims=True)
            weight = jnp.where(valid, jnp.exp(score - peak), 0.0)
            peaks.append(peak)
            totals.append(jnp.sum(weight, axis=1, keepdims=True))
            rounded = (weight * scales[1][n]).astype(jnp.bfloat16)
            sums.append(
                jnp.dot(
                    rounded,
                    quant_ref[0, 1, s, n * BLOCK : (n + 1) * BLOCK, :],
                    preferred_element_type=jnp.float32,
                )
            )
        top = functools.reduce(jnp.maximum, peaks)
        total = jnp.zeros_like(top)
        numer = jnp.zeros((QUERY_GROUP, HEAD_DIM), jnp.float32)
        for n in range(blocks):
            factor = jnp.exp(peaks[n] - top)
            total = total + factor * totals[n]
            numer = numer + factor * sums[n]
        stat_ref[s, 0] = numer
        stat_ref[s, 1] = jnp.where(lane < BLOCK // 2, top, total)


def attend(left, moved, queries, quant, out_shape, unit0):
    owners, units, _, ns, rows, _ = moved.shape
    seq_rows = owners * rows
    blocks = seq_rows // BLOCK
    halves = out_shape[2] // ns
    step_pairs = 2 if ns % 2 == 0 else 1
    steps = ns // step_pairs
    size = units * 2 * ns * seq_rows * HEAD_DIM * 2

    def layer(u):
        return (unit0 + u) // halves

    def place(u, i):
        return ((unit0 + u) % halves) * steps + i

    in_specs = [
        pl.BlockSpec(
            (owners, 1, 2, step_pairs, rows, HEAD_DIM), lambda u, i, left: (0, u, 0, i, 0, 0)
        ),
        pl.BlockSpec(
            (1, step_pairs, QUERY_GROUP, HEAD_DIM),
            lambda u, i, left: (layer(u), place(u, i), 0, 0),
        ),
    ]
    operands = [left, moved, queries]
    aliases = {}
    if quant is not None:
        in_specs.append(pl.BlockSpec(memory_space=pl.ANY))
        operands.append(quant)
        aliases = {3: 0}
    return pl.pallas_call(
        functools.partial(attend_kernel, unit0, halves, ns, step_pairs),
        grid_spec=pltpu.PrefetchScalarGridSpec(
            num_scalar_prefetch=1,
            grid=(units, steps),
            in_specs=in_specs,
            out_specs=[
                pl.BlockSpec(
                    (1, 2, step_pairs, seq_rows, HEAD_DIM),
                    lambda u, i, left: (layer(u), 0, place(u, i), 0, 0),
                ),
                pl.BlockSpec((step_pairs, 2, blocks), lambda u, i, left: (u * steps + i, 0, 0)),
                pl.BlockSpec(
                    (step_pairs, 2, QUERY_GROUP, HEAD_DIM),
                    lambda u, i, left: (u * steps + i, 0, 0, 0),
                ),
            ],
        ),
        out_shape=[
            jax.ShapeDtypeStruct(out_shape, jnp.bfloat16),
            jax.ShapeDtypeStruct((units * ns, 2, blocks), jnp.float32),
            jax.ShapeDtypeStruct((units * ns, 2, QUERY_GROUP, HEAD_DIM), jnp.float32),
        ],
        input_output_aliases=aliases,
        cost_estimate=pl.CostEstimate(
            flops=4 * size * QUERY_GROUP, bytes_accessed=2 * size, transcendentals=0
        ),
        compiler_params=pltpu.CompilerParams(vmem_limit_bytes=48 << 20),
    )(*operands)


def combine_kernel(stat_ref, q_ref, fresh_ref, o_ref, held, send_sem, recv_sem):
    ranges = lax.axis_size("seq")
    me = lax.axis_index("seq")
    amount = stat_ref.shape[0]
    inverse = 1.0 / (float(HEAD_DIM) ** 0.5)
    barrier = pltpu.get_barrier_semaphore()
    for k in range(1, ranges):
        pl.semaphore_signal(
            barrier, inc=1, device_id={"seq": (me + k) % ranges}, device_id_type=MESH
        )
    pl.semaphore_wait(barrier, ranges - 1)
    copies = []
    for k in range(1, ranges):
        copy = pltpu.make_async_remote_copy(
            src_ref=stat_ref,
            dst_ref=held.at[me],
            send_sem=send_sem.at[k - 1],
            recv_sem=recv_sem.at[k - 1],
            device_id={"seq": (me + k) % ranges},
            device_id_type=MESH,
        )
        copy.start()
        copies.append(copy)
    held[me] = stat_ref[...]
    for copy in copies:
        copy.wait()

    def one(i, carry):
        query = q_ref[i].astype(jnp.float32)
        fresh_key = fresh_ref[i, 0:1, :]
        fresh_value = fresh_ref[i, 1:2, :]
        own = jnp.sum(query * fresh_key, axis=1, keepdims=True) * inverse
        tails = [held[r, i, 1] for r in range(ranges)]
        tops = [tail[:, 0:1] for tail in tails]
        top = functools.reduce(jnp.maximum, tops, own)
        own_weight = jnp.exp(own - top)
        numer = own_weight * fresh_value
        denom = own_weight
        for r in range(ranges):
            factor = jnp.exp(tops[r] - top)
            numer = numer + factor * held[r, i, 0]
            denom = denom + factor * tails[r][:, BLOCK // 2 : BLOCK // 2 + 1]
        o_ref[i] = (numer / denom).astype(jnp.bfloat16)
        return carry

    lax.fori_loop(0, amount, one, 0)


def combine(stat, queries, fresh, ident):
    amount = stat.shape[0]
    ranges = lax.axis_size("seq")
    return pl.pallas_call(
        combine_kernel,
        in_specs=[pl.BlockSpec(memory_space=pltpu.VMEM)] * 3,
        out_specs=pl.BlockSpec(memory_space=pltpu.VMEM),
        out_shape=jax.ShapeDtypeStruct((amount, QUERY_GROUP, HEAD_DIM), jnp.bfloat16),
        scratch_shapes=[
            pltpu.VMEM((ranges, *stat.shape), jnp.float32),
            pltpu.SemaphoreType.DMA((ranges - 1,)),
            pltpu.SemaphoreType.DMA((ranges - 1,)),
        ],
        cost_estimate=pl.CostEstimate(
            flops=0, bytes_accessed=stat.size * 4 * ranges, transcendentals=0
        ),
        compiler_params=pltpu.CompilerParams(
            collective_id=ident, has_side_effects=True, vmem_limit_bytes=16 << 20
        ),
    )(stat, queries, fresh)


def on_device(kv_cache, queries, fresh_key_value, lengths):
    layers, _, batch, rows, width = kv_cache.shape
    heads = width // HEAD_DIM
    owners = lax.axis_size("blk")
    pairs = heads * batch // owners
    seq_rows = rows * owners
    blocks = seq_rows // BLOCK
    first_pair = lax.axis_index("blk") * pairs
    left = lengths[(first_pair + jnp.arange(pairs, dtype=jnp.int32)) % batch]
    left = left - lax.axis_index("seq") * seq_rows
    grouped = queries.reshape(layers, pairs, QUERY_GROUP, HEAD_DIM)
    out_shape = (layers, 2, pairs, seq_rows, HEAD_DIM)
    halves = 2 if pairs % 2 == 0 else 1
    ns = pairs // halves
    units = layers * halves - 1

    moved, tail = hand_over(kv_cache, units, ns)
    tail = lax.all_to_all(tail, "blk", split_axis=0, concat_axis=0, tiled=True)
    quant, scale, stat = attend(left, moved, grouped, None, out_shape, 0)
    quant, last_scale, last_stat = attend(left, tail[:, None], grouped, quant, out_shape, units)
    grouped = grouped.reshape(layers * pairs, QUERY_GROUP, HEAD_DIM)
    fresh = fresh_key_value.transpose(0, 2, 1, 3).astype(jnp.float32)
    fresh = fresh.reshape(layers * pairs, 2, HEAD_DIM)
    cut = units * ns
    attended = jnp.concatenate(
        [
            combine(stat, grouped[:cut], fresh[:cut], 0),
            combine(last_stat, grouped[cut:], fresh[cut:], 1),
        ],
        axis=0,
    ).reshape(layers, pairs, QUERY_GROUP * HEAD_DIM)
    block_scale = jnp.concatenate([scale, last_scale], axis=0)
    block_scale = block_scale.reshape(layers, pairs, 2, blocks).transpose(0, 2, 1, 3)
    return quant, block_scale, attended


def solution(mesh):
    in_specs = (
        P(None, None, None, ("seq", "blk"), None),
        P(None, "blk", None),
        P(None, None, "blk", None),
        P(),
    )
    out_specs = (
        P(None, None, "blk", "seq", None),
        P(None, None, "blk", "seq"),
        P(None, "blk", None),
    )
    return jax.shard_map(
        on_device, mesh=mesh, in_specs=in_specs, out_specs=out_specs, check_vma=False
    )
```
